32 devices in a mesh: seq: 8 (over z, x), head: 4 (over y, core).
Axes of the slice: x: 2, y: 2, z: 4, core: 2. Of those that a mesh axis runs over, the one named last changes fastest.
Arguments:
- tokens: bfloat16 [1024, 7168], P('seq', 'head'), may hold values from -6 to 6
- latent_down: bfloat16 [7168, 576], P('head'), may hold values from -0.0625 to 0.0625
- latent_gain: float32 [512], replicated, may hold values from 0.5 to 1.5
- query_nope: bfloat16 [1024, 8192], P('seq', 'head'), may hold values from -200 to 200
- query_rope: bfloat16 [1024, 4096], P('seq', 'head'), may hold values from -6 to 6
- key_up: bfloat16 [64, 128, 512], P('head'), may hold values from -0.5 to 0.5
- value_up: bfloat16 [64, 512, 128], P('head'), may hold values from -0.25 to 0.25
- prefix_latent: bfloat16 [512, 576], P('seq'), may hold values from -6 to 6
- prefix_length: int32 [1], replicated, may hold values from 256 to 512
- page_table: int32 [64], replicated, may hold values from 0 to 63, each once
Outputs:
- attended: bfloat16 [1024, 8192], P('seq', 'head')
- decode_pool: bfloat16 [64, 9216], P('seq')
The draws below stay inside these ranges and needn't reach their ends.
Inputs may be any that keep to these rules, and one draw needn't show every extreme that they name: The prefix rows from prefix_length[0] on are not live. `page_table`: A permutation of the 64 decode slots.
All inputs are finite; a program needn't handle non-finite values.
Results may differ from the reference program's by a relative error of at most 0.015.
Values may be sent and summed in bfloat16 or wider, within the bound.
No kernel may reach another device: no remote copies, remote signals or barrier semaphores. Data moves between devices by JAX's collectives and lax.ppermute only.
A program may use at most 128 MiB of HBM per device.

```python
import jax
import jax.numpy as jnp
from jax import lax

D = 7168
LATENT = 512
ROPE = 64
NOPE = 128
VHEAD = 128
HEADS = 64
PAGE = 16
TOK_DEV = 128
TOKENS = 1024
PREFIX = 512
PAGES = 64
N_SEQ = 8


def draw_query_nope(key, part):
    first_key = jax.random.fold_in(jax.random.fold_in(key, 17), 0)
    values = jax.random.normal(first_key, (TOKENS, HEADS, NOPE), jnp.float32)
    values = jnp.clip(values, -6.0, 6.0)
    return values.reshape(TOKENS, HEADS * NOPE).astype(jnp.bfloat16)


def steps_of(stream_key, dims, shards, smallest, largest):
    gain, own = 1.0, jax.random.fold_in(stream_key, 6)
    for position, blocks in shards:
        draws = jnp.exp(jax.random.uniform(jax.random.fold_in(own, position), (blocks,), jnp.float32, smallest / len(shards), largest / len(shards)))
        gain = gain * jnp.repeat(draws, dims[position] // blocks).reshape([-1 if axis == position else 1 for axis in range(len(dims))])
    return gain


def gaussian(own_key, extent, scale, limit, cuts=(), kind=jnp.bfloat16):
    entries = scale * jax.random.normal(own_key, extent, jnp.float32)
    if cuts:
        entries = entries * steps_of(own_key, extent, cuts, -0.22, 0.18)
    return jnp.clip(entries, -limit, limit).astype(kind)


def setup_inputs(seed: int = 0) -> dict:
    seeds = jax.random.split(jax.random.key(seed), 11)
    tokens = gaussian(seeds[0], (TOKENS, D), 1.0, 6.0, ((0, 8), (1, 4)))
    latent_down = gaussian(seeds[1], (D, LATENT + ROPE), D ** -0.5, 0.0625, ((0, 4),))
    latent_gain = jnp.clip(1.0 + 0.1 * jax.random.normal(seeds[2], (LATENT,), jnp.float32), 0.5, 1.5)
    query_nope = draw_query_nope(jax.random.fold_in(seeds[10], 71), 0)
    query_rope = gaussian(seeds[4], (TOKENS, HEADS * ROPE), 1.0, 6.0, ((0, 8), (1, 4)))
    key_up = gaussian(seeds[5], (HEADS, NOPE, LATENT), NOPE ** -0.5, 0.5, ((0, 4),))
    value_up = gaussian(seeds[6], (HEADS, LATENT, VHEAD), LATENT ** -0.5, 0.25, ((0, 4),))
    prefix_latent = gaussian(seeds[7], (PREFIX, LATENT + ROPE), 1.0, 6.0, ((0, 8),))
    prefix_length = jax.random.randint(seeds[8], (1,), PREFIX // 2, PREFIX + 1).astype(jnp.int32)
    page_table = jax.random.permutation(seeds[9], PAGES).astype(jnp.int32)
    return {"tokens": tokens, "latent_down": latent_down, "latent_gain": latent_gain, "query_nope": query_nope, "query_rope": query_rope, "key_up": key_up, "value_up": value_up, "prefix_latent": prefix_latent, "prefix_length": prefix_length, "page_table": page_table}


def angles(positions):
    half_width = ROPE // 2
    frequency = 10000.0 ** (-jnp.arange(half_width, dtype=jnp.float32) / half_width)
    return positions.astype(jnp.float32)[:, None] * frequency[None, :]

def rotate(values, angle_table):
    half_width = values.shape[-1] // 2
    first = values[..., :half_width]
    second = values[..., half_width:]
    cosine = jnp.cos(angle_table)
    sinus = jnp.sin(angle_table)
    return jnp.concatenate([first * cosine - second * sinus, first * sinus + second * cosine], axis=-1)

def finish(mixed, latent_gain, positions):
    latent = mixed[:, :LATENT]
    rope_part = mixed[:, LATENT:]
    normed = latent * lax.rsqrt(lax.optimization_barrier(jnp.mean(latent * latent, axis=1, keepdims=True)) + 1e-06) * latent_gain
    return jnp.concatenate([normed.astype(jnp.bfloat16), rotate(rope_part, angles(positions)).astype(jnp.bfloat16)], axis=1)

def reference(tokens, latent_down, latent_gain, query_nope, query_rope, key_up, value_up, prefix_latent, prefix_length, page_table):
    offset = prefix_length[0]
    positions = offset + jnp.arange(TOKENS, dtype=jnp.int32)
    mixed = jnp.dot(tokens, latent_down, preferred_element_type=jnp.float32)
    new_keys = finish(mixed, latent_gain, positions)
    all_keys = jnp.concatenate([prefix_latent, new_keys], axis=0).astype(jnp.float32)
    value_rows = all_keys[:, :LATENT]
    lifted = jnp.einsum('thn,hnl->thl', query_nope.reshape(TOKENS, HEADS, NOPE).astype(jnp.float32), key_up.astype(jnp.float32)).astype(jnp.bfloat16)
    turned = rotate(query_rope.reshape(TOKENS, HEADS, ROPE).astype(jnp.float32), angles(positions)[:, None, :]).astype(jnp.bfloat16)
    queries = jnp.concatenate([lifted, turned], axis=2)
    key_index = jnp.arange(PREFIX + TOKENS, dtype=jnp.int32)
    score_scale = (NOPE + ROPE) ** (-0.5)

    def one_block(block_index):
        rows = lax.dynamic_slice_in_dim(queries, block_index * TOK_DEV, TOK_DEV, 0).reshape(TOK_DEV * HEADS, LATENT + ROPE).astype(jnp.float32)
        scores = jnp.dot(all_keys, rows.T, precision=lax.Precision.HIGHEST) * score_scale
        query_token = block_index * TOK_DEV + jnp.arange(TOK_DEV * HEADS, dtype=jnp.int32) // HEADS
        in_prefix = key_index[:, None] < PREFIX
        live_mask = jnp.where(in_prefix, key_index[:, None] < offset, key_index[:, None] - PREFIX <= query_token[None, :])
        best = lax.optimization_barrier(jnp.max(jnp.where(live_mask, scores, -jnp.inf), axis=0))
        weights = jnp.where(live_mask, jnp.exp(scores - best[None, :]), 0.0)
        denominator = lax.optimization_barrier(jnp.sum(weights, axis=0))
        rounded = weights.astype(jnp.bfloat16).astype(jnp.float32)
        summed = lax.dot_general(rounded, value_rows, (((0,), (0,)), ((), ())), precision=lax.Precision.HIGHEST)
        attention = (summed / denominator[:, None]).astype(jnp.bfloat16).reshape(TOK_DEV, HEADS, LATENT)
        output = jnp.einsum('thl,hlv->thv', attention.astype(jnp.float32), value_up.astype(jnp.float32))
        return output.reshape(TOK_DEV, HEADS * VHEAD).astype(jnp.bfloat16)
    attended = lax.map(one_block, jnp.arange(N_SEQ, dtype=jnp.int32)).reshape(TOKENS, HEADS * VHEAD)
    pages = new_keys.reshape(PAGES, PAGE * (LATENT + ROPE))
    decode_pool = jnp.zeros_like(pages).at[page_table].set(pages)
    return (attended, decode_pool)
```

```python
import jax
import jax.numpy as jnp
from jax import lax
from jax.experimental import pallas as pl
from jax.experimental.pallas import tpu as pltpu
from jax.sharding import PartitionSpec as P

LATENT = 512
ROPE = 64
NOPE = 128
VHEAD = 128
PAGE = 16
LANES = 128
WIDE = LATENT + 2 * ROPE
DEAD = -1e30
LOG2E = 1.4426950408889634


def f32_dot(a, b, dims=((1,), (0,))):
    return lax.dot_general(a, b, (dims, ((), ())), preferred_element_type=jnp.float32)


def vmem_spec():
    return pl.BlockSpec(memory_space=pltpu.VMEM)


def smem_spec():
    return pl.BlockSpec(memory_space=pltpu.SMEM)


def params(limit_mib, semantics=None):
    return pltpu.CompilerParams(
        vmem_limit_bytes=limit_mib << 20, dimension_semantics=semantics
    )


def project_kernel(where_ref, tokens_ref, down_ref, keep_ref, send_ref, total):
    step = pl.program_id(0)
    term = f32_dot(tokens_ref[...], down_ref[...])

    @pl.when(step == 0)
    def _():
        total[...] = term

    @pl.when(step > 0)
    def _():
        total[...] += term

    @pl.when(step == pl.num_programs(0) - 1)
    def _():
        half = keep_ref.shape[0]
        core = where_ref[1]
        keep_ref[...] = total[pl.ds(pl.multiple_of(core * half, half), half), :]
        send_ref[...] = total[pl.ds(pl.multiple_of((1 - core) * half, half), half), :]


def project(where, tokens, latent_down):
    rows, depth = tokens.shape
    width = latent_down.shape[1]
    block = 256 if depth % 256 == 0 else depth
    half = jax.ShapeDtypeStruct((rows // 2, width), jnp.float32)
    return pl.pallas_call(
        project_kernel,
        grid=(depth // block,),
        in_specs=[
            smem_spec(),
            pl.BlockSpec((rows, block), lambda k: (0, k)),
            pl.BlockSpec((block, width), lambda k: (k, 0)),
        ],
        out_specs=[pl.BlockSpec((rows // 2, width), lambda k: (0, 0))] * 2,
        out_shape=[half, half],
        scratch_shapes=[pltpu.VMEM((rows, width), jnp.float32)],
        compiler_params=params(16, ("arbitrary",)),
        name="project",
    )(where, tokens, latent_down)


def swap_halves(values):
    lane = lax.broadcasted_iota(jnp.int32, values.shape, 1)
    left = pltpu.roll(values, LANES - ROPE // 2, 1)
    right = pltpu.roll(values, ROPE // 2, 1)
    return jnp.where(lane % ROPE < ROPE // 2, left, right)


def finish_kernel(where_ref, mine_ref, theirs_ref, gain_ref, cos_ref, sin_ref, out_ref):
    half = out_ref.shape[0]
    start = pl.multiple_of(where_ref[1] * half, half)
    mixed = mine_ref[...].astype(jnp.float32) + theirs_ref[...].astype(jnp.float32)
    latent = mixed[:, :LATENT]
    scale = lax.rsqrt(jnp.mean(latent * latent, axis=1, keepdims=True) + 1e-06)
    out_ref[:, :LATENT] = (latent * scale * gain_ref[...]).astype(jnp.bfloat16)
    rope = mixed[:, LATENT:]
    rope = jnp.concatenate([rope, rope], axis=1)
    turned = rope * cos_ref[pl.ds(start, half), :] + swap_halves(rope) * sin_ref[
        pl.ds(start, half), :
    ]
    out_ref[:, LATENT:] = turned.astype(jnp.bfloat16)


def finish(where, mine, theirs, gain, cosine, sinus):
    return pl.pallas_call(
        finish_kernel,
        in_specs=[smem_spec()] + [vmem_spec()] * 5,
        out_specs=vmem_spec(),
        out_shape=jax.ShapeDtypeStruct((mine.shape[0], WIDE), jnp.bfloat16),
        compiler_params=params(8),
        name="finish",
    )(where, mine, theirs, gain, cosine, sinus)


def query_kernel(nope_ref, rope_ref, up_ref, cos_ref, sin_ref, out_ref):
    heads = up_ref.shape[0]
    for pair in range(heads // 2):
        values = rope_ref[:, pair * LANES : (pair + 1) * LANES].astype(jnp.float32)
        turned = (values * cos_ref[...] + swap_halves(values) * sin_ref[...]).astype(jnp.bfloat16)
        lane = lax.broadcasted_iota(jnp.int32, turned.shape, 1)
        for side in range(2):
            head = 2 * pair + side
            lifted = f32_dot(nope_ref[:, head * NOPE : (head + 1) * NOPE], up_ref[head])
            out_ref[head, :, :LATENT] = lifted.astype(jnp.bfloat16)
            live = (lane < ROPE) if side == 0 else (lane >= ROPE)
            out_ref[head, :, LATENT:] = jnp.where(live, turned, jnp.zeros_like(turned))


def absorb(query_nope, query_rope, key_up, cosine, sinus):
    heads = key_up.shape[0]
    rows = query_nope.shape[0]
    group = 4
    return pl.pallas_call(
        query_kernel,
        grid=(heads // group,),
        in_specs=[
            pl.BlockSpec((rows, group * NOPE), lambda g: (0, g)),
            pl.BlockSpec((rows, group * ROPE), lambda g: (0, g)),
            pl.BlockSpec((group, NOPE, LATENT), lambda g: (g, 0, 0)),
            pl.BlockSpec((rows, LANES), lambda g: (0, 0)),
            pl.BlockSpec((rows, LANES), lambda g: (0, 0)),
        ],
        out_specs=pl.BlockSpec((group, rows, WIDE), lambda g: (g, 0, 0)),
        out_shape=jax.ShapeDtypeStruct((heads, rows, WIDE), jnp.bfloat16),
        compiler_params=params(16, ("arbitrary",)),
        name="absorb",
    )(query_nope, query_rope, key_up, cosine, sinus)


def attend_kernel(plan, where_ref, table_ref, q_ref, up_ref, *refs):
    prefix_plan, block_plan, prefix_rows, block_rows = plan
    count = len(prefix_plan) + len(block_plan)
    pieces = refs[:count]
    out_ref, pool_ref, keys, even, odd = refs[count:]
    seq, core, offset = where_ref[0], where_ref[1], where_ref[2]
    heads, rows, _ = q_ref.shape
    total = keys.shape[0]
    chunk = 512 if (prefix_rows % 512 == 0 and block_rows % 512 == 0) else 128

    for (flip, side, start, size, width), piece in zip(prefix_plan + block_plan, pieces):
        is_prefix = width < WIDE
        base = 0 if is_prefix else prefix_rows
        other = core if side == 0 else 1 - core
        place = base + (seq ^ flip) * (2 * size) + other * size
        place = pl.multiple_of(place, size)
        values = piece[start : start + size, :]
        if is_prefix:
            values = jnp.concatenate([values, values[:, LATENT:]], axis=1)
        keys[pl.ds(place, size), :] = values

    factor = (NOPE + ROPE) ** (-0.5) * LOG2E
    group_rows = 2 * rows

    def score(group, store):
        query = q_ref[pl.ds(2 * group, 2)].reshape(group_rows, WIDE)
        for start in range(0, total, chunk):
            values = f32_dot(query, keys[start : start + chunk, :], ((1,), (1,)))
            column = lax.broadcasted_iota(jnp.int32, values.shape, 1)
            if start < prefix_rows:
                live = column < offset - start
            else:
                row = lax.broadcasted_iota(jnp.int32, values.shape, 0) % rows
                live = column - row <= seq * rows - (start - prefix_rows)
            store[:, start : start + chunk] = jnp.where(live, values, DEAD)

    def settle(group, store):
        top = jnp.max(store[...], axis=1, keepdims=True)
        running = jnp.zeros((group_rows, LATENT), jnp.float32)
        denominator = jnp.zeros((group_rows, 1), jnp.float32)
        for start in range(0, total, chunk):
            weights = jnp.exp2((store[:, start : start + chunk] - top) * factor)
            denominator += jnp.sum(weights, axis=1, keepdims=True)
            running += f32_dot(weights.astype(jnp.bfloat16), keys[start : start + chunk, :LATENT])
        attention = (running / denominator).astype(jnp.bfloat16)
        for side in range(2):
            head = 2 * group + side
            values = f32_dot(attention[side * rows : (side + 1) * rows], up_ref[head])
            at = pl.multiple_of(head * VHEAD, VHEAD)
            out_ref[:, pl.ds(at, VHEAD)] = values.astype(jnp.bfloat16)

    score(0, even)

    def advance(index, carry):
        score(2 * index + 1, odd)
        settle(2 * index, even)
        following = jnp.minimum(2 * index + 2, heads // 2 - 1)
        score(following, even)
        settle(2 * index + 1, odd)
        return carry

    lax.fori_loop(0, heads // 4, advance, 0)

    slots = pool_ref.shape[0]
    table = table_ref[...]
    wanted = lax.broadcasted_iota(jnp.int32, (slots, table.shape[1]), 0) + seq * slots
    page = lax.broadcasted_iota(jnp.int32, (slots, table.shape[1]), 1)
    mine = jnp.sum(jnp.where(table == wanted, page, 0), axis=1, keepdims=True)
    token = lax.broadcasted_iota(jnp.int32, (slots, block_rows), 1)
    picks = [
        jnp.where(token == mine * PAGE + row, 1.0, 0.0) for row in range(PAGE)
    ]
    pick = jnp.concatenate(picks, axis=0).astype(jnp.bfloat16)
    found = f32_dot(pick, keys[prefix_rows:, :])
    row_width = LATENT + ROPE
    for pair in range(PAGE // 2):
        first = found[2 * pair * slots : (2 * pair + 1) * slots, :row_width]
        second = found[(2 * pair + 1) * slots : (2 * pair + 2) * slots, :row_width]
        both = jnp.concatenate([first, second], axis=1).astype(jnp.bfloat16)
        pool_ref[:, pair * 2 * row_width : (pair + 1) * 2 * row_width] = both


def attend(where, table, queries, value_up, prefix_parts, block_parts, block_rows, slots):
    heads, rows, _ = queries.shape
    prefix_plan, block_plan, pieces = [], [], []
    prefix_rows = 0
    for plan, parts in ((prefix_plan, prefix_parts), (block_plan, block_parts)):
        for side, flips, values in parts:
            size = values.shape[0] // len(flips)
            for index, flip in enumerate(flips):
                plan.append((flip, side, index * size, size, values.shape[1]))
                pieces.append(values)
                if plan is prefix_plan:
                    prefix_rows += size
    plan = (prefix_plan, block_plan, prefix_rows, block_rows)
    total = prefix_rows + block_rows

    def body(*refs):
        attend_kernel(plan, *refs)

    return pl.pallas_call(
        body,
        in_specs=[smem_spec()] + [vmem_spec()] * (3 + len(pieces)),
        out_specs=[vmem_spec(), vmem_spec()],
        out_shape=[
            jax.ShapeDtypeStruct((rows, heads * VHEAD), jnp.bfloat16),
            jax.ShapeDtypeStruct((slots, PAGE * (LATENT + ROPE)), jnp.bfloat16),
        ],
        scratch_shapes=[
            pltpu.VMEM((total, WIDE), jnp.bfloat16),
            pltpu.VMEM((2 * rows, total), jnp.float32),
            pltpu.VMEM((2 * rows, total), jnp.float32),
        ],
        compiler_params=params(48),
        name="attend",
    )(where, table, queries, value_up, *pieces)


def solution(mesh):
    seq_count = mesh.shape["seq"]
    head_count = mesh.shape["head"]

    def seq_flip(values, flip):
        return lax.ppermute(values, "seq", [(i, i ^ flip) for i in range(seq_count)])

    def head_flip(values, flip):
        return lax.ppermute(values, "head", [(i, i ^ flip) for i in range(head_count)])

    def gather(values):
        flips, held = [0], values
        bit = seq_count // 2
        while bit > 2:
            held = jnp.concatenate([held, seq_flip(held, bit)], axis=0)
            flips = flips + [f ^ bit for f in flips]
            bit //= 2
        parts = [(flips, held)]
        for flip in range(1, 2 * bit):
            parts.append(([f ^ flip for f in flips], seq_flip(held, flip)))
        mine = [(0, f, v) for f, v in parts]
        return mine + [(1, f, head_flip(v, 1)) for f, v in parts]

    def per_device(
        tokens,
        latent_down,
        latent_gain,
        query_nope,
        query_rope,
        key_up,
        value_up,
        prefix_latent,
        prefix_length,
        page_table,
    ):
        rows = tokens.shape[0]
        half_width = ROPE // 2
        seq = lax.axis_index("seq")
        core = lax.axis_index("head") % 2
        where = jnp.stack([seq, core, prefix_length[0]]).astype(jnp.int32)
        positions = prefix_length[0] + seq * rows + jnp.arange(rows, dtype=jnp.int32)
        frequency = 10000.0 ** (-jnp.arange(half_width, dtype=jnp.float32) / half_width)
        angle = positions.astype(jnp.float32)[:, None] * jnp.tile(frequency, 4)[None, :]
        sign = jnp.tile(jnp.repeat(jnp.array([-1.0, 1.0], jnp.float32), half_width), 2)
        cosine, sinus = jnp.cos(angle), jnp.sin(angle) * sign[None, :]

        keep, send = project(where, tokens, latent_down)
        mixed = keep + head_flip(send, 1)
        bit = 2
        while bit < head_count:
            mixed = mixed.astype(jnp.bfloat16)
            if 2 * bit < head_count:
                mixed = mixed.astype(jnp.float32) + head_flip(mixed, bit).astype(jnp.float32)
            else:
                new_rows = finish(
                    where, mixed, head_flip(mixed, bit), latent_gain[None, :], cosine, sinus
                )
            bit *= 2

        queries = absorb(query_nope, query_rope, key_up, cosine, sinus)
        shared = prefix_latent.shape[0] // 2
        prefix_mine = lax.dynamic_slice_in_dim(prefix_latent, core * shared, shared, 0)
        prefix_parts = gather(prefix_mine)
        block_parts = gather(new_rows)
        attended, pool = attend(
            where,
            page_table[None, :],
            queries,
            value_up,
            prefix_parts,
            block_parts,
            rows * seq_count,
            rows // PAGE,
        )
        return attended, pool

    placed = (
        P("seq", "head"),
        P("head", None),
        P(),
        P("seq", "head"),
        P("seq", "head"),
        P("head", None, None),
        P("head", None, None),
        P("seq", None),
        P(),
        P(),
    )
    return jax.shard_map(
        per_device,
        mesh=mesh,
        in_specs=placed,
        out_specs=(P("seq", "head"), P("seq", None)),
        check_vma=False,
    )
```

```python
import jax
import jax.numpy as jnp
from jax import lax
from jax.experimental import pallas as pl
from jax.experimental.pallas import tpu as pltpu
from jax.sharding import PartitionSpec as P

LATENT = 512
ROPE = 64
NOPE = 128
VHEAD = 128
PAGE = 16
LANES = 128
WIDE = LATENT + 2 * ROPE
DEEP = WIDE + LANES
DEAD = -1e30
LOG2E = 1.4426950408889634


def f32_dot(a, b, dims=((1,), (0,))):
    return lax.dot_general(a, b, (dims, ((), ())), preferred_element_type=jnp.float32)


def vmem_spec():
    return pl.BlockSpec(memory_space=pltpu.VMEM)


def smem_spec():
    return pl.BlockSpec(memory_space=pltpu.SMEM)


def hbm_spec():
    return pl.BlockSpec(memory_space=pltpu.HBM)


def stay(values):
    return pltpu.with_memory_space_constraint(values, pltpu.HBM)


def params(limit_mib):
    return pltpu.CompilerParams(vmem_limit_bytes=limit_mib << 20)


def project_kernel(where_ref, tokens_hbm, down_hbm, keep_ref, send_ref, tokens, down, total, sems):
    width = down.shape[0]
    cuts = list(range(0, width, 2 * LANES)) + [width]
    copies = [pltpu.make_async_copy(tokens_hbm, tokens, sems.at[0])]
    for index in range(len(cuts) - 1):
        at = pl.ds(cuts[index], cuts[index + 1] - cuts[index])
        copies.append(
            pltpu.make_async_copy(down_hbm.at[at], down.at[at], sems.at[index + 1])
        )
    for copy in copies:
        copy.start()
    copies[0].wait()
    for index in range(len(cuts) - 1):
        copies[index + 1].wait()
        at = slice(cuts[index], cuts[index + 1])
        total[:, at] = f32_dot(tokens[...], down[at, :], ((1,), (1,)))
    half = keep_ref.shape[0]
    core = where_ref[1]
    keep_ref[...] = total[pl.ds(pl.multiple_of(core * half, half), half), :]
    send_ref[...] = total[pl.ds(pl.multiple_of((1 - core) * half, half), half), :]


def project(where, tokens, down_turned):
    rows = tokens.shape[0]
    width = down_turned.shape[0]
    half = jax.ShapeDtypeStruct((rows // 2, width), jnp.float32)
    count = 1 + pl.cdiv(width, 2 * LANES)
    return pl.pallas_call(
        project_kernel,
        in_specs=[smem_spec(), hbm_spec(), hbm_spec()],
        out_specs=[vmem_spec()] * 2,
        out_shape=[half, half],
        scratch_shapes=[
            pltpu.VMEM(tokens.shape, tokens.dtype),
            pltpu.VMEM(down_turned.shape, down_turned.dtype),
            pltpu.VMEM((rows, width), jnp.float32),
            pltpu.SemaphoreType.DMA((count,)),
        ],
        compiler_params=params(12),
        name="project",
    )(where, stay(tokens), stay(down_turned))


def swap_halves(values):
    lane = lax.broadcasted_iota(jnp.int32, values.shape, 1)
    left = pltpu.roll(values, LANES - ROPE // 2, 1)
    right = pltpu.roll(values, ROPE // 2, 1)
    return jnp.where(lane % ROPE < ROPE // 2, left, right)


def finish_kernel(where_ref, mine_ref, theirs_ref, gain_ref, cos_ref, sin_ref, out_ref):
    half = out_ref.shape[0]
    start = pl.multiple_of(where_ref[1] * half, half)
    mixed = mine_ref[...].astype(jnp.float32) + theirs_ref[...].astype(jnp.float32)
    latent = mixed[:, :LATENT]
    scale = lax.rsqrt(jnp.mean(latent * latent, axis=1, keepdims=True) + 1e-06)
    out_ref[:, :LATENT] = (latent * scale * gain_ref[...]).astype(jnp.bfloat16)
    rope = mixed[:, LATENT:]
    rope = jnp.concatenate([rope, rope], axis=1)
    turned = rope * cos_ref[pl.ds(start, half), :] + swap_halves(rope) * sin_ref[
        pl.ds(start, half), :
    ]
    out_ref[:, LATENT:] = turned.astype(jnp.bfloat16)


def finish(where, mine, theirs, gain, cosine, sinus):
    return pl.pallas_call(
        finish_kernel,
        in_specs=[smem_spec()] + [vmem_spec()] * 5,
        out_specs=vmem_spec(),
        out_shape=jax.ShapeDtypeStruct((mine.shape[0], WIDE), jnp.bfloat16),
        compiler_params=params(4),
        name="finish",
    )(where, mine, theirs, gain, cosine, sinus)


def absorb_kernel(nope_hbm, rope_hbm, up_hbm, cos_ref, sin_ref, out_ref, nope, rope, up, sems):
    heads, rows, _ = out_ref.shape
    group = 4
    count = heads // group

    def copies(index):
        heads_at = pl.ds(index * group, group)
        nope_at = pl.ds(pl.multiple_of(index * group * NOPE, LANES), group * NOPE)
        rope_at = pl.ds(pl.multiple_of(index * group * ROPE, LANES), group * ROPE)
        return (
            pltpu.make_async_copy(up_hbm.at[heads_at], up.at[heads_at], sems.at[0, index]),
            pltpu.make_async_copy(nope_hbm.at[:, nope_at], nope.at[index], sems.at[1, index]),
            pltpu.make_async_copy(rope_hbm.at[:, rope_at], rope.at[index], sems.at[2, index]),
        )

    for index in range(count):
        for copy in copies(index):
            copy.start()
    row = lax.broadcasted_iota(jnp.int32, (rows, LANES), 0)
    lane = lax.broadcasted_iota(jnp.int32, (rows, LANES), 1)
    marks = jnp.where(row == lane, 1.0, 0.0).astype(jnp.bfloat16)

    def advance(index, carry):
        for copy in copies(index):
            copy.wait()
        for pair in range(group // 2):
            values = rope[index, :, pair * LANES : (pair + 1) * LANES].astype(jnp.float32)
            turned = values * cos_ref[...] + swap_halves(values) * sin_ref[...]
            for side in range(2):
                local = 2 * pair + side
                head = index * group + local
                lifted = f32_dot(nope[index, :, local * NOPE : (local + 1) * NOPE], up[head])
                out_ref[head, :, :LATENT] = lifted.astype(jnp.bfloat16)
                live = (lane < ROPE) if side == 0 else (lane >= ROPE)
                out_ref[head, :, LATENT:WIDE] = jnp.where(live, turned, 0.0).astype(jnp.bfloat16)
                out_ref[head, :, WIDE:] = marks
        return carry

    lax.fori_loop(0, count, advance, 0)


def absorb(query_nope, query_rope, key_up, cosine, sinus):
    heads = key_up.shape[0]
    rows = query_nope.shape[0]
    group = 4
    count = heads // group
    return pl.pallas_call(
        absorb_kernel,
        in_specs=[hbm_spec()] * 3 + [vmem_spec()] * 2,
        out_specs=vmem_spec(),
        out_shape=jax.ShapeDtypeStruct((heads, rows, DEEP), jnp.bfloat16),
        scratch_shapes=[
            pltpu.VMEM((count, rows, group * NOPE), jnp.bfloat16),
            pltpu.VMEM((count, rows, group * ROPE), jnp.bfloat16),
            pltpu.VMEM(key_up.shape, jnp.bfloat16),
            pltpu.SemaphoreType.DMA((3, count)),
        ],
        compiler_params=params(16),
        cost_estimate=pl.CostEstimate(
            flops=2 * heads * rows * NOPE * LATENT,
            transcendentals=0,
            bytes_accessed=8 * heads * rows * DEEP,
        ),
        name="absorb",
    )(stay(query_nope), stay(query_rope), stay(key_up), cosine, sinus)


def piece_source(piece, seq, core):
    _, _, _, flip, side = piece
    return seq ^ flip, (core if side == 0 else 1 - core)


def lay_keys(keys, at, piece, refs, seq, core, offset, rows):
    array, start, size, _, _ = piece
    source, half = piece_source(piece, seq, core)
    values = refs[array][start : start + size, :]
    row = lax.broadcasted_iota(jnp.int32, (size, LANES), 0)
    lane = lax.broadcasted_iota(jnp.int32, (size, LANES), 1)
    if values.shape[1] < WIDE:
        values = jnp.concatenate([values, values[:, LATENT:]], axis=1)
        dead = row + (2 * source + half) * size >= offset
    else:
        dead = row - lane > (seq - source) * rows - half * size
    keys[at : at + size, :WIDE] = values
    keys[at : at + size, WIDE:] = jnp.where(dead, DEAD, 0.0).astype(jnp.bfloat16)


def over_lanes(values, width):
    return jnp.concatenate([values] * (width // LANES), axis=1)


SCALE = (NOPE + ROPE) ** (-0.5) * LOG2E


def score(store, query, keys):
    total = store.shape[1]
    chunk = 2 * LANES
    for start in range(0, total, chunk):
        store[:, start : start + chunk] = f32_dot(query, keys[start : start + chunk, :], ((1,), (1,)))


def weigh(store, keys, top, denominator):
    rows, total = store.shape
    chunk = 2 * LANES
    best = store[:, :LANES]
    for start in range(LANES, total, LANES):
        best = jnp.maximum(best, store[:, start : start + LANES])
    best = jnp.broadcast_to(jnp.max(best, axis=1, keepdims=True), (rows, LANES))
    fade = None
    if top is not None:
        best = jnp.maximum(best, top)
        fade = jnp.exp2((top - best) * SCALE)
        denominator = denominator * fade
    running = None
    for start in range(0, total, chunk):
        parts = []
        for at in range(start, start + chunk, LANES):
            weights = jnp.exp2((store[:, at : at + LANES] - best) * SCALE)
            denominator = weights if denominator is None else denominator + weights
            parts.append(weights.astype(jnp.bfloat16))
        update = f32_dot(
            jnp.concatenate(parts, axis=1), keys[start : start + chunk, :LATENT]
        )
        running = update if running is None else running + update
    return best, denominator, fade, running


def early_kernel(pieces, where_ref, q_ref, *refs):
    arrays = refs[:-6]
    top_ref, sum_ref, run_ref, keys, left, right = refs[-6:]
    seq, core, offset = where_ref[0], where_ref[1], where_ref[2]
    heads, rows, _ = q_ref.shape
    at = 0
    for piece in pieces:
        lay_keys(keys, at, piece, arrays, seq, core, offset, rows)
        at += piece[2]

    def advance(index, carry):
        for side, store in enumerate((left, right)):
            query = q_ref[pl.ds(4 * index + 2 * side, 2)].reshape(2 * rows, DEEP)
            score(store, query, keys)
        for side, store in enumerate((left, right)):
            where = pl.ds(pl.multiple_of((2 * index + side) * 2 * rows, 2 * rows), 2 * rows)
            best, denominator, _, running = weigh(store, keys, None, None)
            top_ref[where, :] = best
            sum_ref[where, :] = denominator
            run_ref[where, :] = running
        return carry

    lax.fori_loop(0, heads // 4, advance, 0)


def late_kernel(pieces, spare, where_ref, table_ref, q_ref, up_ref, top_ref, sum_ref, run_ref, *refs):
    arrays = refs[:-5]
    out_ref, pool_ref, keys, left, right = refs[-5:]
    seq, core, offset = where_ref[0], where_ref[1], where_ref[2]
    heads, rows, _ = q_ref.shape
    used = left.shape[1]
    at = 0
    for piece in pieces + spare:
        lay_keys(keys, at, piece, arrays, seq, core, offset, rows)
        at += piece[2]

    def advance(index, carry):
        for side, store in enumerate((left, right)):
            query = q_ref[pl.ds(4 * index + 2 * side, 2)].reshape(2 * rows, DEEP)
            score(store, query, keys)
        for side, store in enumerate((left, right)):
            where = pl.ds(pl.multiple_of((2 * index + side) * 2 * rows, 2 * rows), 2 * rows)
            _, denominator, fade, running = weigh(store, keys, top_ref[where, :], sum_ref[where, :])
            running = running + run_ref[where, :] * over_lanes(fade, LATENT)
            denominator = jnp.sum(denominator, axis=1, keepdims=True)
            inverse = 1.0 / jnp.broadcast_to(denominator, (2 * rows, LANES))
            attention = (running * over_lanes(inverse, LATENT)).astype(jnp.bfloat16)
            for half in range(2):
                head = 4 * index + 2 * side + half
                values = f32_dot(attention[half * rows : (half + 1) * rows], up_ref[head])
                to = pl.multiple_of(head * VHEAD, VHEAD)
                out_ref[:, pl.ds(to, VHEAD)] = values.astype(jnp.bfloat16)
        return carry

    lax.fori_loop(0, heads // 4, advance, 0)

    slots = pool_ref.shape[0]
    table = table_ref[...]
    wanted = lax.broadcasted_iota(jnp.int32, table.shape, 0) * 0 + seq * slots
    slot = lax.broadcasted_iota(jnp.int32, (slots, table.shape[1]), 0)
    page = lax.broadcasted_iota(jnp.int32, (slots, table.shape[1]), 1)
    mine = jnp.sum(jnp.where(table - wanted == slot, page, 0), axis=1, keepdims=True)
    tokens = []
    for piece in pieces + spare:
        source, half = piece_source(piece, seq, core)
        token = lax.broadcasted_iota(jnp.int32, (slots, piece[2]), 1)
        tokens.append(token + (source * rows + half * piece[2]))
    place = jnp.concatenate(tokens, axis=1) - mine * PAGE
    picks = [jnp.where(place == row, 1.0, 0.0) for row in range(PAGE)]
    pick = jnp.concatenate(picks, axis=0).astype(jnp.bfloat16)
    found = f32_dot(pick, keys[:, :WIDE])
    row_width = LATENT + ROPE
    for pair in range(PAGE // 2):
        first = found[2 * pair * slots : (2 * pair + 1) * slots, :row_width]
        second = found[(2 * pair + 1) * slots : (2 * pair + 2) * slots, :row_width]
        both = jnp.concatenate([first, second], axis=1).astype(jnp.bfloat16)
        pool_ref[:, pair * 2 * row_width : (pair + 1) * 2 * row_width] = both


def cut(parts, arrays):
    pieces = []
    for side, flips, values in parts:
        size = values.shape[0] // len(flips)
        for index, flip in enumerate(flips):
            pieces.append((len(arrays), index * size, size, flip, side))
        arrays.append(values)
    return pieces


def rows_of(pieces):
    return sum(piece[2] for piece in pieces)


def attend_cost(queries, count):
    heads, rows, _ = queries.shape
    return pl.CostEstimate(
        flops=2 * heads * rows * count * (DEEP + LATENT),
        transcendentals=heads * rows * count,
        bytes_accessed=4 * heads * rows * DEEP,
    )


def attend_early(where, queries, parts):
    heads, rows, _ = queries.shape
    arrays = []
    pieces = cut(parts, arrays)
    count = rows_of(pieces)

    def body(*refs):
        early_kernel(pieces, *refs)

    lane_state = jax.ShapeDtypeStruct((heads * rows, LANES), jnp.float32)
    return pl.pallas_call(
        body,
        in_specs=[smem_spec()] + [vmem_spec()] * (1 + len(arrays)),
        out_specs=[vmem_spec()] * 3,
        out_shape=[
            lane_state,
            lane_state,
            jax.ShapeDtypeStruct((heads * rows, LATENT), jnp.float32),
        ],
        scratch_shapes=[
            pltpu.VMEM((count, DEEP), jnp.bfloat16),
            pltpu.VMEM((2 * rows, count), jnp.float32),
            pltpu.VMEM((2 * rows, count), jnp.float32),
        ],
        compiler_params=params(20 + 8 * pl.cdiv(count, 1024)),
        cost_estimate=attend_cost(queries, count),
        name="early",
    )(where, queries, *arrays)


def attend_late(where, table, queries, value_up, state, parts, spare_parts, slots):
    heads, rows, _ = queries.shape
    arrays = []
    pieces = cut(parts, arrays)
    spare = cut(spare_parts, arrays)
    count = rows_of(pieces)

    def body(*refs):
        late_kernel(pieces, spare, *refs)

    return pl.pallas_call(
        body,
        in_specs=[smem_spec()] + [vmem_spec()] * (6 + len(arrays)),
        out_specs=[vmem_spec(), vmem_spec()],
        out_shape=[
            jax.ShapeDtypeStruct((rows, heads * VHEAD), jnp.bfloat16),
            jax.ShapeDtypeStruct((slots, PAGE * (LATENT + ROPE)), jnp.bfloat16),
        ],
        scratch_shapes=[
            pltpu.VMEM((count + rows_of(spare), DEEP), jnp.bfloat16),
            pltpu.VMEM((2 * rows, count), jnp.float32),
            pltpu.VMEM((2 * rows, count), jnp.float32),
        ],
        compiler_params=params(20 + 8 * pl.cdiv(count, 1024)),
        cost_estimate=attend_cost(queries, count),
        name="late",
    )(where, table, queries, value_up, *state, *arrays)


def solution(mesh):
    seq_count = mesh.shape["seq"]
    head_count = mesh.shape["head"]

    def seq_flip(values, flip):
        return lax.ppermute(values, "seq", [(i, i ^ flip) for i in range(seq_count)])

    def head_flip(values, flip):
        return lax.ppermute(values, "head", [(i, i ^ flip) for i in range(head_count)])

    def gather(values):
        flips, held = [0], values
        bit = seq_count // 2
        while bit > 2:
            held = jnp.concatenate([held, seq_flip(held, bit)], axis=0)
            flips = flips + [f ^ bit for f in flips]
            bit //= 2
        rest = [([f ^ flip for f in flips], seq_flip(held, flip)) for flip in range(1, 2 * bit)]
        near = [(0, flips, held), (1, flips, head_flip(held, 1))]
        far = [(0, f, v) for f, v in rest] + [(1, f, head_flip(v, 1)) for f, v in rest]
        return near, far

    def per_device(
        tokens,
        latent_down,
        latent_gain,
        query_nope,
        query_rope,
        key_up,
        value_up,
        prefix_latent,
        prefix_length,
        page_table,
    ):
        rows = tokens.shape[0]
        half_width = ROPE // 2
        seq = lax.axis_index("seq")
        core = lax.axis_index("head") % 2
        where = jnp.stack([seq, core, prefix_length[0]]).astype(jnp.int32)
        positions = prefix_length[0] + seq * rows + jnp.arange(rows, dtype=jnp.int32)
        frequency = 10000.0 ** (-jnp.arange(half_width, dtype=jnp.float32) / half_width)
        angle = positions.astype(jnp.float32)[:, None] * jnp.tile(frequency, 4)[None, :]
        sign = jnp.tile(jnp.repeat(jnp.array([-1.0, 1.0], jnp.float32), half_width), 2)
        cosine, sinus = jnp.cos(angle), jnp.sin(angle) * sign[None, :]

        keep, send = project(where, tokens, latent_down.T)
        mixed = keep + head_flip(send, 1)
        bit = 2
        while bit < head_count:
            mixed = mixed.astype(jnp.bfloat16)
            if 2 * bit < head_count:
                mixed = mixed.astype(jnp.float32) + head_flip(mixed, bit).astype(jnp.float32)
            else:
                new_rows = finish(
                    where, mixed, head_flip(mixed, bit), latent_gain[None, :], cosine, sinus
                )
            bit *= 2

        queries = absorb(query_nope, query_rope, key_up, cosine, sinus)
        shared = prefix_latent.shape[0] // 2
        prefix_mine = lax.dynamic_slice_in_dim(prefix_latent, core * shared, shared, 0)
        prefix_near, prefix_far = gather(prefix_mine)
        near, far = gather(new_rows)
        state = attend_early(where, queries, prefix_near + prefix_far + near)
        attended, pool = attend_late(
            where, page_table[None, :], queries, value_up, state, far, near, rows // PAGE
        )
        return attended, pool

    placed = (
        P("seq", "head"),
        P("head", None),
        P(),
        P("seq", "head"),
        P("seq", "head"),
        P("head", None, None),
        P("head", None, None),
        P("seq", None),
        P(),
        P(),
    )
    return jax.shard_map(
        per_device,
        mesh=mesh,
        in_specs=placed,
        out_specs=(P("seq", "head"), P("seq", None)),
        check_vma=False,
    )
```

```python
import jax
import jax.numpy as jnp
from jax import lax
from jax.experimental import pallas as pl
from jax.experimental.pallas import tpu as pltpu
from jax.sharding import PartitionSpec as P


LATENT = 512
ROPE = 64
NOPE = 128
VHEAD = 128
PAGE = 16
LANES = 128
WIDE = LATENT + 2 * ROPE
DEEP = WIDE + LANES
DEAD = -1e30
LOG2E = 1.4426950408889634


def f32_dot(a, b, dims=((1,), (0,))):
    return lax.dot_general(a, b, (dims, ((), ())), preferred_element_type=jnp.float32)


def vmem_spec():
    return pl.BlockSpec(memory_space=pltpu.VMEM)


def hbm_spec():
    return pl.BlockSpec(memory_space=pltpu.HBM)


def stay(values):
    return pltpu.with_memory_space_constraint(values, pltpu.HBM)


def params(limit_mib):
    return pltpu.CompilerParams(vmem_limit_bytes=limit_mib << 20)


def project_kernel(tokens_hbm, down_hbm, keep_ref, send_ref, tokens, down, total, sems):
    width = down.shape[0]
    cuts = list(range(0, width, 2 * LANES)) + [width]
    copies = [pltpu.make_async_copy(tokens_hbm, tokens, sems.at[0])]
    for index in range(len(cuts) - 1):
        at = pl.ds(cuts[index], cuts[index + 1] - cuts[index])
        copies.append(
            pltpu.make_async_copy(down_hbm.at[at], down.at[at], sems.at[index + 1])
        )
    for copy in copies:
        copy.start()
    copies[0].wait()
    for index in range(len(cuts) - 1):
        copies[index + 1].wait()
        at = slice(cuts[index], cuts[index + 1])
        total[:, at] = f32_dot(tokens[...], down[at, :], ((1,), (1,)))
    half = keep_ref.shape[0]
    core = lax.axis_index("head") % 2
    keep_ref[...] = total[pl.ds(pl.multiple_of(core * half, half), half), :]
    send_ref[...] = total[pl.ds(pl.multiple_of((1 - core) * half, half), half), :]


def project(tokens, down_turned):
    rows = tokens.shape[0]
    width = down_turned.shape[0]
    half = jax.ShapeDtypeStruct((rows // 2, width), jnp.float32)
    count = 1 + pl.cdiv(width, 2 * LANES)
    return pl.pallas_call(
        project_kernel,
        in_specs=[hbm_spec(), hbm_spec()],
        out_specs=[vmem_spec()] * 2,
        out_shape=[half, half],
        scratch_shapes=[
            pltpu.VMEM(tokens.shape, tokens.dtype),
            pltpu.VMEM(down_turned.shape, down_turned.dtype),
            pltpu.VMEM((rows, width), jnp.float32),
            pltpu.SemaphoreType.DMA((count,)),
        ],
        compiler_params=params(12),
        name="project",
    )(stay(tokens), stay(down_turned))


def swap_halves(values):
    lane = lax.broadcasted_iota(jnp.int32, values.shape, 1)
    left = pltpu.roll(values, LANES - ROPE // 2, 1)
    right = pltpu.roll(values, ROPE // 2, 1)
    return jnp.where(lane % ROPE < ROPE // 2, left, right)


def finish_kernel(mine_ref, theirs_ref, gain_ref, cos_ref, sin_ref, out_ref):
    half = out_ref.shape[0]
    start = pl.multiple_of(lax.axis_index("head") % 2 * half, half)
    mixed = mine_ref[...].astype(jnp.float32) + theirs_ref[...].astype(jnp.float32)
    latent = mixed[:, :LATENT]
    scale = lax.rsqrt(jnp.mean(latent * latent, axis=1, keepdims=True) + 1e-06)
    out_ref[:, :LATENT] = (latent * scale * gain_ref[...]).astype(jnp.bfloat16)
    rope = mixed[:, LATENT:]
    rope = jnp.concatenate([rope, rope], axis=1)
    turned = rope * cos_ref[pl.ds(start, half), :] + swap_halves(rope) * sin_ref[
        pl.ds(start, half), :
    ]
    out_ref[:, LATENT:] = turned.astype(jnp.bfloat16)


def finish(mine, theirs, gain, cosine, sinus):
    return pl.pallas_call(
        finish_kernel,
        in_specs=[vmem_spec()] * 5,
        out_specs=vmem_spec(),
        out_shape=jax.ShapeDtypeStruct((mine.shape[0], WIDE), jnp.bfloat16),
        compiler_params=params(4),
        name="finish",
    )(mine, theirs, gain, cosine, sinus)


def absorb_kernel(nope_hbm, rope_hbm, up_hbm, cos_ref, sin_ref, out_ref, nope, rope, up, sems):
    heads, rows, _ = out_ref.shape
    group = 4
    count = heads // group

    def copies(index):
        heads_at = pl.ds(index * group, group)
        nope_at = pl.ds(pl.multiple_of(index * group * NOPE, LANES), group * NOPE)
        rope_at = pl.ds(pl.multiple_of(index * group * ROPE, LANES), group * ROPE)
        return (
            pltpu.make_async_copy(up_hbm.at[heads_at], up.at[heads_at], sems.at[0, index]),
            pltpu.make_async_copy(nope_hbm.at[:, nope_at], nope.at[index], sems.at[1, index]),
            pltpu.make_async_copy(rope_hbm.at[:, rope_at], rope.at[index], sems.at[2, index]),
        )

    for index in range(count):
        for copy in copies(index):
            copy.start()
    row = lax.broadcasted_iota(jnp.int32, (rows, LANES), 0)
    lane = lax.broadcasted_iota(jnp.int32, (rows, LANES), 1)
    marks = jnp.where(row == lane, 1.0, 0.0).astype(jnp.bfloat16)

    def advance(index, carry):
        for copy in copies(index):
            copy.wait()
        for pair in range(group // 2):
            values = rope[index, :, pair * LANES : (pair + 1) * LANES].astype(jnp.float32)
            turned = values * cos_ref[...] + swap_halves(values) * sin_ref[...]
            for side in range(2):
                local = 2 * pair + side
                head = index * group + local
                lifted = f32_dot(nope[index, :, local * NOPE : (local + 1) * NOPE], up[head])
                out_ref[head, :, :LATENT] = lifted.astype(jnp.bfloat16)
                live = (lane < ROPE) if side == 0 else (lane >= ROPE)
                out_ref[head, :, LATENT:WIDE] = jnp.where(live, turned, 0.0).astype(jnp.bfloat16)
                out_ref[head, :, WIDE:] = marks
        return carry

    lax.fori_loop(0, count, advance, 0)


def absorb(query_nope, query_rope, key_up, cosine, sinus):
    heads = key_up.shape[0]
    rows = query_nope.shape[0]
    group = 4
    count = heads // group
    return pl.pallas_call(
        absorb_kernel,
        in_specs=[hbm_spec()] * 3 + [vmem_spec()] * 2,
        out_specs=vmem_spec(),
        out_shape=jax.ShapeDtypeStruct((heads, rows, DEEP), jnp.bfloat16),
        scratch_shapes=[
            pltpu.VMEM((count, rows, group * NOPE), jnp.bfloat16),
            pltpu.VMEM((count, rows, group * ROPE), jnp.bfloat16),
            pltpu.VMEM(key_up.shape, jnp.bfloat16),
            pltpu.SemaphoreType.DMA((3, count)),
        ],
        compiler_params=params(16),
        cost_estimate=pl.CostEstimate(
            flops=2 * heads * rows * NOPE * LATENT,
            transcendentals=0,
            bytes_accessed=8 * heads * rows * DEEP,
        ),
        name="absorb",
    )(stay(query_nope), stay(query_rope), stay(key_up), cosine, sinus)


def piece_source(piece, seq, core):
    _, _, _, flip, side = piece
    return seq ^ flip, (core if side == 0 else 1 - core)


def lay_keys(keys, at, piece, refs, seq, core, offset, rows):
    array, start, size, _, _ = piece
    source, half = piece_source(piece, seq, core)
    values = refs[array][start : start + size, :]
    row = lax.broadcasted_iota(jnp.int32, (size, LANES), 0)
    lane = lax.broadcasted_iota(jnp.int32, (size, LANES), 1)
    if values.shape[1] < WIDE:
        values = jnp.concatenate([values, values[:, LATENT:]], axis=1)
        dead = offset[:1, :] - row <= (2 * source + half) * size
    else:
        dead = row - lane > (seq - source) * rows - half * size
    keys[at : at + size, :WIDE] = values
    keys[at : at + size, WIDE:] = jnp.where(dead, DEAD, 0.0).astype(jnp.bfloat16)


def over_lanes(values, width):
    return jnp.concatenate([values] * (width // LANES), axis=1)


SCALE = (NOPE + ROPE) ** (-0.5) * LOG2E


def score(store, query, keys):
    total = store.shape[1]
    chunk = 2 * LANES
    for start in range(0, total, chunk):
        store[:, start : start + chunk] = f32_dot(query, keys[start : start + chunk, :], ((1,), (1,)))


def weigh(store, keys, top, denominator):
    rows, total = store.shape
    chunk = 2 * LANES
    best = store[:, :LANES]
    for start in range(LANES, total, LANES):
        best = jnp.maximum(best, store[:, start : start + LANES])
    best = jnp.broadcast_to(jnp.max(best, axis=1, keepdims=True), (rows, LANES))
    fade = None
    if top is not None:
        best = jnp.maximum(best, top)
        fade = jnp.exp2((top - best) * SCALE)
        denominator = denominator * fade
    running = None
    for start in range(0, total, chunk):
        parts = []
        for at in range(start, start + chunk, LANES):
            weights = jnp.exp2((store[:, at : at + LANES] - best) * SCALE)
            denominator = weights if denominator is None else denominator + weights
            parts.append(weights.astype(jnp.bfloat16))
        update = f32_dot(
            jnp.concatenate(parts, axis=1), keys[start : start + chunk, :LATENT]
        )
        running = update if running is None else running + update
    return best, denominator, fade, running


def early_kernel(pieces, offset_ref, q_ref, *refs):
    arrays = refs[:-6]
    top_ref, sum_ref, run_ref, keys, left, right = refs[-6:]
    seq, core = lax.axis_index("seq"), lax.axis_index("head") % 2
    heads, rows, _ = q_ref.shape
    at = 0
    for piece in pieces:
        lay_keys(keys, at, piece, arrays, seq, core, offset_ref[...], rows)
        at += piece[2]

    def advance(index, carry):
        for side, store in enumerate((left, right)):
            query = q_ref[pl.ds(4 * index + 2 * side, 2)].reshape(2 * rows, DEEP)
            score(store, query, keys)
        for side, store in enumerate((left, right)):
            where = pl.ds(pl.multiple_of((2 * index + side) * 2 * rows, 2 * rows), 2 * rows)
            best, denominator, _, running = weigh(store, keys, None, None)
            top_ref[where, :] = best
            sum_ref[where, :] = denominator
            run_ref[where, :] = running
        return carry

    lax.fori_loop(0, heads // 4, advance, 0)


def pick_pages(pool, table, pieces, keys, seq, core, rows):
    slots = pool.shape[0]
    slot = lax.broadcasted_iota(jnp.int32, (slots, table.shape[1]), 0)
    page = lax.broadcasted_iota(jnp.int32, (slots, table.shape[1]), 1)
    mine = jnp.sum(jnp.where(table - seq * slots == slot, page, 0), axis=1, keepdims=True)
    tokens = []
    for piece in pieces:
        source, half = piece_source(piece, seq, core)
        token = lax.broadcasted_iota(jnp.int32, (slots, piece[2]), 1)
        tokens.append(token + (source * rows + half * piece[2]))
    place = jnp.concatenate(tokens, axis=1) - mine * PAGE
    picks = [jnp.where(place == row, 1.0, 0.0) for row in range(PAGE)]
    pick = jnp.concatenate(picks, axis=0).astype(jnp.bfloat16)
    found = f32_dot(pick, keys[:, :WIDE])
    width = LATENT + ROPE
    for pair in range(PAGE // 2):
        first = found[2 * pair * slots : (2 * pair + 1) * slots, :width]
        second = found[(2 * pair + 1) * slots : (2 * pair + 2) * slots, :width]
        both = jnp.concatenate([first, second], axis=1).astype(jnp.bfloat16)
        pool[:, pair * 2 * width : (pair + 1) * 2 * width] = both


def late_kernel(pieces, spare, table_ref, q_ref, up_ref, top_ref, sum_ref, run_ref, *refs):
    arrays = refs[:-8]
    out_hbm, pool_hbm, keys, left, right, out, pool, sems = refs[-8:]
    seq, core = lax.axis_index("seq"), lax.axis_index("head") % 2
    heads, rows, _ = q_ref.shape
    at = 0
    for piece in pieces + spare:
        lay_keys(keys, at, piece, arrays, seq, core, None, rows)
        at += piece[2]

    pick_pages(pool, table_ref[...], pieces + spare, keys, seq, core, rows)
    pool_copy = pltpu.make_async_copy(pool, pool_hbm, sems.at[0])
    pool_copy.start()
    count = heads // 4

    def out_copy(index):
        to = pl.ds(pl.multiple_of(index * 4 * VHEAD, 4 * VHEAD), 4 * VHEAD)
        return pltpu.make_async_copy(out.at[index], out_hbm.at[:, to], sems.at[1 + index])

    def advance(index, carry):
        for side, store in enumerate((left, right)):
            query = q_ref[pl.ds(4 * index + 2 * side, 2)].reshape(2 * rows, DEEP)
            score(store, query, keys)
        for side, store in enumerate((left, right)):
            where = pl.ds(pl.multiple_of((2 * index + side) * 2 * rows, 2 * rows), 2 * rows)
            _, denominator, fade, running = weigh(store, keys, top_ref[where, :], sum_ref[where, :])
            running = running + run_ref[where, :] * over_lanes(fade, LATENT)
            denominator = jnp.sum(denominator, axis=1, keepdims=True)
            inverse = 1.0 / jnp.broadcast_to(denominator, (2 * rows, LANES))
            attention = (running * over_lanes(inverse, LATENT)).astype(jnp.bfloat16)
            for half in range(2):
                local = 2 * side + half
                values = f32_dot(attention[half * rows : (half + 1) * rows], up_ref[4 * index + local])
                out[index, :, local * VHEAD : (local + 1) * VHEAD] = values.astype(jnp.bfloat16)
        out_copy(index).start()
        return carry

    lax.fori_loop(0, count, advance, 0)
    for index in range(count):
        out_copy(index).wait()
    pool_copy.wait()


def cut(parts, arrays):
    pieces = []
    for side, flips, values in parts:
        size = values.shape[0] // len(flips)
        for index, flip in enumerate(flips):
            pieces.append((len(arrays), index * size, size, flip, side))
        arrays.append(values)
    return pieces


def rows_of(pieces):
    return sum(piece[2] for piece in pieces)


def attend_cost(queries, count):
    heads, rows, _ = queries.shape
    return pl.CostEstimate(
        flops=2 * heads * rows * count * (DEEP + LATENT),
        transcendentals=heads * rows * count,
        bytes_accessed=4 * heads * rows * DEEP,
    )


def attend_early(offset, queries, parts):
    heads, rows, _ = queries.shape
    arrays = []
    pieces = cut(parts, arrays)
    count = rows_of(pieces)

    def body(*refs):
        early_kernel(pieces, *refs)

    lane_state = jax.ShapeDtypeStruct((heads * rows, LANES), jnp.float32)
    return pl.pallas_call(
        body,
        in_specs=[vmem_spec()] * (2 + len(arrays)),
        out_specs=[vmem_spec()] * 3,
        out_shape=[
            lane_state,
            lane_state,
            jax.ShapeDtypeStruct((heads * rows, LATENT), jnp.float32),
        ],
        scratch_shapes=[
            pltpu.VMEM((count, DEEP), jnp.bfloat16),
            pltpu.VMEM((2 * rows, count), jnp.float32),
            pltpu.VMEM((2 * rows, count), jnp.float32),
        ],
        compiler_params=params(20 + 8 * pl.cdiv(count, 1024)),
        cost_estimate=attend_cost(queries, count),
        name="early",
    )(offset, queries, *arrays)


def attend_late(table, queries, value_up, state, parts, spare_parts, slots):
    heads, rows, _ = queries.shape
    arrays = []
    pieces = cut(parts, arrays)
    spare = cut(spare_parts, arrays)
    count = rows_of(pieces)

    def body(*refs):
        late_kernel(pieces, spare, *refs)

    return pl.pallas_call(
        body,
        in_specs=[vmem_spec()] * (6 + len(arrays)),
        out_specs=[hbm_spec(), hbm_spec()],
        out_shape=[
            jax.ShapeDtypeStruct((rows, heads * VHEAD), jnp.bfloat16),
            jax.ShapeDtypeStruct((slots, PAGE * (LATENT + ROPE)), jnp.bfloat16),
        ],
        scratch_shapes=[
            pltpu.VMEM((count + rows_of(spare), DEEP), jnp.bfloat16),
            pltpu.VMEM((2 * rows, count), jnp.float32),
            pltpu.VMEM((2 * rows, count), jnp.float32),
            pltpu.VMEM((heads // 4, rows, 4 * VHEAD), jnp.bfloat16),
            pltpu.VMEM((slots, PAGE * (LATENT + ROPE)), jnp.bfloat16),
            pltpu.SemaphoreType.DMA((1 + heads // 4,)),
        ],
        compiler_params=params(20 + 8 * pl.cdiv(count, 1024)),
        cost_estimate=attend_cost(queries, count),
        name="late",
    )(table, queries, value_up, *state, *arrays)


def solution(mesh):
    seq_count = mesh.shape["seq"]
    head_count = mesh.shape["head"]

    def seq_flip(values, flip):
        return lax.ppermute(values, "seq", [(i, i ^ flip) for i in range(seq_count)])

    def head_flip(values, flip):
        return lax.ppermute(values, "head", [(i, i ^ flip) for i in range(head_count)])

    def gather(values):
        flips, held = [0], values
        bit = seq_count // 2
        while bit > 2:
            held = jnp.concatenate([held, seq_flip(held, bit)], axis=0)
            flips = flips + [f ^ bit for f in flips]
            bit //= 2
        rest = []
        for flip in range(1, 2 * bit):
            rest.append(([f ^ flip for f in flips], seq_flip(held, flip)))
        near = [(0, flips, held), (1, flips, head_flip(held, 1))]
        far = [(0, f, v) for f, v in rest] + [(1, f, head_flip(v, 1)) for f, v in rest]
        return near, far

    def compute(
        tokens,
        latent_down,
        latent_gain,
        query_nope,
        query_rope,
        key_up,
        value_up,
        prefix_latent,
        prefix_length,
        page_table,
    ):
        rows = tokens.shape[0]
        half_width = ROPE // 2
        seq = lax.axis_index("seq")
        core = lax.axis_index("head") % 2
        positions = prefix_length[0] + seq * rows + jnp.arange(rows, dtype=jnp.int32)
        frequency = 10000.0 ** (-jnp.arange(half_width, dtype=jnp.float32) / half_width)
        angle = positions.astype(jnp.float32)[:, None] * jnp.tile(frequency, 4)[None, :]
        sign = jnp.tile(jnp.repeat(jnp.array([-1.0, 1.0], jnp.float32), half_width), 2)
        cosine, sinus = jnp.cos(angle), jnp.sin(angle) * sign[None, :]
        offset = jnp.broadcast_to(prefix_length[0], (8, LANES))

        shared = prefix_latent.shape[0] // 2
        prefix_mine = lax.dynamic_slice_in_dim(prefix_latent, core * shared, shared, 0)
        prefix_near, prefix_far = gather(prefix_mine)

        keep, send = project(tokens, latent_down.T)
        mixed = keep + head_flip(send, 1)
        bit = 2
        while bit < head_count:
            mixed = mixed.astype(jnp.bfloat16)
            theirs = head_flip(mixed, bit)
            if 2 * bit < head_count:
                mixed = mixed.astype(jnp.float32) + theirs.astype(jnp.float32)
            bit *= 2
        new_rows = finish(mixed, theirs, latent_gain[None, :], cosine, sinus)

        queries = absorb(query_nope, query_rope, key_up, cosine, sinus)
        near, far = gather(new_rows)
        state = attend_early(offset, queries, prefix_near + prefix_far + near)
        attended, pool = attend_late(
            page_table[None, :], queries, value_up, state, far, near, rows // PAGE
        )
        return attended, pool

    placed = (
        P("seq", "head"),
        P("head", None),
        P(),
        P("seq", "head"),
        P("seq", "head"),
        P("head", None, None),
        P("head", None, None),
        P("seq", None),
        P(),
        P(),
    )
    return jax.shard_map(
        compute,
        mesh=mesh,
        in_specs=placed,
        out_specs=(P("seq", "head"), P("seq", None)),
        check_vma=False,
    )
```
